256 devices in a mesh: groups: 2 (over y), dp: 32 (over z, core), expert: 4 (over x).
Axes of the slice: x: 4, y: 2, z: 16, core: 2. Of those that a mesh axis runs over, the one named last changes fastest.
The devices are a block of a 4x16x16 slice.
Arguments:
- queries: bfloat16 [2, 1024, 32, 128], P(None, ('groups', 'dp'), 'expert'), parts along dimension 1, may hold values from -6 to 6
- fresh_kv: bfloat16 [2, 1024, 4, 256], P(None, ('groups', 'dp'), 'expert'), parts along dimension 1, may hold values from -6 to 6
- kv_pool: bfloat16 [20480, 16, 4, 256], P(('groups', 'dp'), None, 'expert'), parts along dimension 0, may hold values from -6 to 6
- page_table: int32 [1024, 305], P(('groups', 'dp')), parts along dimension 0, may hold values from -1 to 319, as said below
- context_lengths: int32 [1024], P(('groups', 'dp')), parts along dimension 0, may hold values from 1 to 4880, as said below
- residual: bfloat16 [2, 1024, 4096], P(None, ('groups', 'dp'), 'expert'), parts along dimension 1, may hold values from -16 to 16
- out_weight: bfloat16 [4096, 4096], P('expert', 'dp'), may hold values from -0.09375 to 0.09375
- norm_gain: float32 [4096], P('expert'), may hold values from 0.1 to 1.9
- expert_ids: int32 [2, 1024, 8], P(None, ('groups', 'dp')), parts along dimension 1, may hold values from 0 to 63, all different within a row; in each aligned block of 16 rows (0 to 15, 16 to 31, ..., all dimensions but the last counted through in order) at most 5 rows name the same one
- route_weights: float32 [2, 1024, 8], P(None, ('groups', 'dp')), parts along dimension 1, may hold values from 0.1 to 1
- gate_up: bfloat16 [64, 2, 4096, 768], P('dp', None, 'expert'), may hold values from -0.09375 to 0.09375
- down_proj: bfloat16 [64, 768, 4096], P('dp', None, 'expert'), may hold values from -0.21875 to 0.21875
Outputs:
- layer_out: bfloat16 [2, 1024, 4096], P(None, ('groups', 'dp'), 'expert'), parts along dimension 1
The draws below stay inside these ranges and needn't reach their ends.
There are 2 independent parts, one for each index of `groups`. The reference program is written for one: setup_inputs(seed, part) draws one part's arguments, and reference() takes and returns one part's arrays. A program takes and returns all parts, laid end to end along the dimension named above; an argument that names none is the same for every part. Nothing has to cross between parts.
Inputs may be any that keep to these rules, and one draw needn't show every extreme that they name: `page_table`: entries 0 to ceil(context_lengths[i] / 16) - 1 of a row name distinct pages, no page is named twice within the 16 requests of one block, and later entries are -1. The requests of one block hold at most 320 pages together; in every draw some block holds exactly 320, and some request holds exactly 305 pages. `context_lengths`: every request holds at least one cached token; in every draw some request holds exactly 4880. `expert_ids`: within the rows of one device (16 requests of one step) no expert is named by more than 5 rows.
All inputs are finite; a program needn't handle non-finite values.
Results may differ from the reference program's by a relative error of at most 0.005.
Values may be sent and summed in bfloat16 or wider, within the bound.
A program may use at most 64 MiB of HBM per device.

```python
import math
import jax
import jax.numpy as jnp
import numpy as np
from jax import lax

D = 4096
HQ = 32
KVH = 4
HD = 128
HID = 768
TOP = 8
PAGE = 16
STEPS = 2
REQ_DP = 16
REQS = 512
EXPERTS = 64
POOL = 320
POOL_ALL = 10240
MAXP = 305
CAP = 5
N_DP = 32


def device_layout(device_key, page_total, packed):
    first_key, second_key, third_key = jax.random.split(device_key, 3)
    scores = jax.random.permutation(first_key, POOL).astype(jnp.int32)
    index = jnp.arange(POOL, dtype=jnp.int32)
    allowed = (index >= 1) & (index < page_total)
    ranked = jnp.where(allowed, scores, POOL + index)
    picked = jnp.argsort(ranked, stable=True)[:REQ_DP - 1]
    spread_cuts = jnp.sort(picked).astype(jnp.int32)
    packed_cuts = jnp.arange(1, REQ_DP, dtype=jnp.int32)
    cuts = jnp.where(packed, packed_cuts, spread_cuts).astype(jnp.int32)
    bounds = jnp.concatenate([jnp.zeros((1,), jnp.int32), cuts, jnp.reshape(page_total, (1,)).astype(jnp.int32)])
    counts = bounds[1:] - bounds[:-1]
    order = jax.random.permutation(second_key, POOL).astype(jnp.int32)
    slot_index = jnp.arange(MAXP, dtype=jnp.int32)
    where_in = bounds[:-1, None] + slot_index[None, :]
    live_slot = slot_index[None, :] < counts[:, None]
    table = jnp.where(live_slot, order[jnp.clip(where_in, 0, POOL - 1)], -1).astype(jnp.int32)
    tail = jax.random.randint(third_key, (REQ_DP,), 1, PAGE + 1).astype(jnp.int32)
    last_request = jnp.arange(REQ_DP, dtype=jnp.int32) == REQ_DP - 1
    tail = jnp.where(packed & last_request, PAGE, tail).astype(jnp.int32)
    lengths = ((counts - 1) * PAGE + tail).astype(jnp.int32)
    return (lengths, table)


def pool_layout(key):
    base = jax.random.fold_in(key, 11)
    level_key, busy_key, device_key = jax.random.split(base, 3)
    levels = jax.random.randint(level_key, (N_DP,), 1, 9).astype(jnp.int32)
    busiest = jax.random.randint(busy_key, (), 0, N_DP)
    is_busiest = jnp.arange(N_DP) == busiest
    levels = jnp.where(is_busiest, 8, levels)
    totals = (POOL * levels // 8).astype(jnp.int32)
    device_keys = jax.random.split(device_key, N_DP)
    lengths, table = jax.vmap(device_layout)(device_keys, totals, is_busiest)
    return (lengths.reshape(REQS), table.reshape(REQS, MAXP))


def draw_context_lengths(key, part):
    return pool_layout(key)[0]


def draw_page_table(key, part):
    return pool_layout(key)[1]


def draw_kv_pool(key, part):
    shape = (POOL_ALL, PAGE, KVH, 2 * HD)
    values = jnp.clip(jax.random.normal(jax.random.fold_in(key, 31), shape, jnp.float32), -6.0, 6.0)
    return values.astype(jnp.bfloat16)


def draw_queries(key, part):
    shape = (STEPS, REQS, HQ, HD)
    values = jnp.clip(jax.random.normal(jax.random.fold_in(key, 41), shape, jnp.float32), -6.0, 6.0)
    return values.astype(jnp.bfloat16)


def draw_residual(key, part):
    shape = (STEPS, REQS, D)
    feature = jnp.arange(D, dtype=jnp.float32) / D
    row_scale = jnp.exp(jax.random.uniform(jax.random.fold_in(key, 52), (STEPS, REQS, 1), jnp.float32, math.log(0.3), math.log(3.0)))
    col_scale = jnp.exp(jax.random.uniform(jax.random.fold_in(key, 53), (D,), jnp.float32, -0.35, 0.35))
    noise = jax.random.normal(jax.random.fold_in(key, 51), shape, jnp.float32)
    ramp = jnp.exp(math.log(0.4) + (math.log(2.0) - math.log(0.4)) * feature)
    return jnp.clip(noise * row_scale * col_scale * ramp, -16.0, 16.0).astype(jnp.bfloat16)


def level_of(stream_key, extent, shards, low, largest):
    gain = 1.0
    for axis_at, parts in shards:
        draws = jax.random.uniform(jax.random.fold_in(jax.random.fold_in(stream_key, 6), axis_at), (parts,), jnp.float32, low / len(shards), largest / len(shards))
        gain = gain * jnp.repeat(jnp.exp(draws), extent[axis_at] // parts).reshape((-1,) + (1,) * (len(extent) - 1 - axis_at))
    return gain


def deal_out(rng, own, number, rows, amount, top, limit, slope):
    order = jax.random.permutation(rng, amount)
    heavy_load, ordinary = load_shares(amount, rows * top, limit, slope, True), load_shares(amount, rows * top, limit, slope, False)
    places = jnp.arange(amount)

    def named(sizes, turn):
        used = int((sizes > 0).sum())
        fixed = max(1, used // 4)
        passed = fixed + (places - fixed + turn * (used - fixed)) % max(1, amount - fixed)
        return jnp.zeros((amount,), jnp.int32).at[order[jnp.where(places < fixed, places, passed)]].set(jnp.asarray(sizes, jnp.int32))

    sizes = jnp.where(number % 4 == 0, named(heavy_load, number // 4), named(ordinary, number - number // 4 - 1))
    mixed = jax.random.permutation(jax.random.fold_in(own, 3), amount)
    giver, sink = mixed[0:amount // 2 * 2:2], mixed[1:amount // 2 * 2:2]
    room = jnp.minimum(sizes[giver] - 1, limit - sizes[sink]) // 2
    room = jnp.where((giver == order[0]) | (sink == order[0]) | (sizes[sink] == 0), 0, jnp.maximum(room, 0))
    passed = jax.random.randint(jax.random.fold_in(own, 4), (amount // 2,), 0, 1 << 20) % (room + 1)
    sizes = sizes.at[giver].add(-passed).at[sink].add(passed)
    members = jnp.searchsorted(jnp.cumsum(sizes), jnp.arange(rows * top), side="right").astype(jnp.int32)
    table = members.reshape(top, rows).T
    table = table[jax.random.permutation(jax.random.fold_in(own, 1), rows)]
    turn = jax.random.randint(jax.random.fold_in(own, 2), (rows, 1), 0, top)
    return jnp.take_along_axis(table, (jnp.arange(top)[None, :] + turn) % top, axis=1)


def load_shares(amount, total, limit, slope, full):
    loads = [(1 << 20) // math.isqrt(standing ** slope) + 1 for standing in range(1, amount + 1)]
    largest = limit if full else min(limit, max(-(-total // amount), total * loads[0] // sum(loads)))
    least = 1 if total - largest >= amount - 1 else 0
    given, spare = [largest] + [least] * (amount - 1), total - largest - least * (amount - 1)
    while spare > 0:
        movable = [i for i in range(1, amount) if given[i] < largest] or [i for i in range(1, amount) if given[i] < limit]
        pool, budget = sum([loads[i] for i in movable]), spare
        for i in movable:
            addition = min(limit - given[i], max(1, budget * loads[i] // pool), spare)
            given[i] = given[i] + addition
            spare = spare - addition
    return np.array(given)


def gaussian(own_key, dims, scale, bound, cuts=(), kind=jnp.bfloat16):
    array = scale * jax.random.normal(own_key, dims, jnp.float32)
    if cuts:
        array = array * level_of(own_key, dims, cuts, -0.22, 0.18)
    return jnp.clip(array, -bound, bound).astype(kind)


def setup_inputs(seed: int = 0, part: int = 0) -> dict:
    arg_keys = jax.random.split(jax.random.key(seed), 13)
    part_splits = jax.random.split(jax.random.fold_in(arg_keys[12], part), 13)
    queries = draw_queries(jax.random.fold_in(jax.random.fold_in(arg_keys[12], part), 71), part)
    fresh_kv = gaussian(part_splits[1], (STEPS, REQS, KVH, 2 * HD), 1.0, 6.0, ((1, 32), (2, 4)))
    kv_pool = draw_kv_pool(jax.random.fold_in(jax.random.fold_in(arg_keys[12], part), 71), part)
    page_table = draw_page_table(jax.random.fold_in(jax.random.fold_in(arg_keys[12], part), 71), part)
    context_lengths = draw_context_lengths(jax.random.fold_in(jax.random.fold_in(arg_keys[12], part), 71), part)
    residual = draw_residual(jax.random.fold_in(jax.random.fold_in(arg_keys[12], part), 71), part)
    out_weight = gaussian(arg_keys[6], (HQ * HD, D), (HQ * HD) ** -0.5, 0.09375, ((0, 4), (1, 32)))
    norm_gain = jnp.clip(1.0 + 0.18 * jax.random.normal(arg_keys[7], (D,), jnp.float32), 0.1, 1.9)
    expert_ids_keys = jax.random.split(jax.random.fold_in(part_splits[8], 1), STEPS * REQS // REQ_DP)
    expert_ids_turns = jax.random.permutation(jax.random.fold_in(part_splits[8], 3), STEPS * REQS // REQ_DP)
    expert_ids = jax.vmap(lambda own, number: deal_out(jax.random.fold_in(part_splits[8], 2), own, number, REQ_DP, EXPERTS, TOP, CAP, 2))(expert_ids_keys, expert_ids_turns).reshape((STEPS, REQS, TOP))
    route_weights = jnp.clip(jnp.exp(math.log(1.0) - 2.3025851 * jax.random.uniform(part_splits[9], (STEPS, REQS, TOP), jnp.float32) ** level_of(part_splits[9], (STEPS, REQS, TOP), ((1, 32),), -0.2, 0.2)), 0.1, 1.0)
    gate_up = gaussian(arg_keys[10], (EXPERTS, 2, D, HID), D ** -0.5, 0.09375, ((0, 32), (2, 4)))
    down_proj = gaussian(arg_keys[11], (EXPERTS, HID, D), HID ** -0.5, 0.21875, ((0, 32), (2, 4)))
    return dict(queries=queries, fresh_kv=fresh_kv, kv_pool=kv_pool, page_table=page_table, context_lengths=context_lengths, residual=residual, out_weight=out_weight, norm_gain=norm_gain, expert_ids=expert_ids, route_weights=route_weights, gate_up=gate_up, down_proj=down_proj)


NEG = -1e+30
EPS = 1e-06
EXACT = lax.Precision.HIGHEST

def page_owners(table, lengths, pool_pages, page_len):
    pages = jnp.arange(pool_pages, dtype=jnp.int32)
    matches = table[:, :, None] == pages[None, None, :]
    ownership = jnp.any(matches, axis=1)
    slot_index = jnp.arange(table.shape[1], dtype=jnp.int32)
    position = lax.optimization_barrier(jnp.sum(jnp.where(matches, slot_index[None, :, None], 0), axis=(0, 1)))
    owner_length = lax.optimization_barrier(jnp.sum(jnp.where(ownership, lengths[:, None], 0), axis=0))
    live_count = jnp.clip(owner_length - position * page_len, 0, page_len)
    return (ownership, live_count)

def attend(query_block, fresh_block, pool_block, table_block, length_block):
    step_count, req_count, head_count, head_width = query_block.shape
    pool_pages, page_len, kv_heads, _ = pool_block.shape
    group_size = head_count // kv_heads
    score_scale = 1.0 / jnp.sqrt(jnp.float32(head_width))
    ownership, live_count = page_owners(table_block, length_block, pool_pages, page_len)
    owned_f = ownership.astype(jnp.float32)
    grouped = query_block.reshape(step_count, req_count, kv_heads, group_size, head_width).astype(jnp.float32)
    page_query = jnp.einsum('rp,srkgd->pskgd', owned_f, grouped, precision=EXACT)
    key_rows = pool_block[..., :head_width].astype(jnp.float32)
    value_rows = pool_block[..., head_width:].astype(jnp.float32)
    page_scores = jnp.einsum('pskgd,ptkd->pskgt', page_query, key_rows) * score_scale
    in_page = jnp.arange(page_len)[None, :] < live_count[:, None]
    page_scores = jnp.where(in_page[:, None, None, None, :], page_scores, NEG)
    fresh_keys = fresh_block[..., :head_width].astype(jnp.float32)
    fresh_values = fresh_block[..., head_width:].astype(jnp.float32)
    fresh_scores = jnp.einsum('srkgd,urkd->srkgu', grouped, fresh_keys) * score_scale
    causal = jnp.arange(step_count)[:, None] >= jnp.arange(step_count)[None, :]
    fresh_scores = jnp.where(causal[:, None, None, None, :], fresh_scores, NEG)
    page_best = lax.optimization_barrier(jnp.max(page_scores, axis=4))
    row_best = lax.optimization_barrier(jnp.max(jnp.where(ownership[:, :, None, None, None], page_best[None], NEG), axis=1))
    row_best = jnp.maximum(row_best, jnp.moveaxis(lax.optimization_barrier(jnp.max(fresh_scores, axis=4)), 0, 1))
    owner_best = jnp.einsum('rp,rskg->pskg', owned_f, row_best, precision=EXACT)
    page_probs = jnp.exp(page_scores - owner_best[..., None])
    page_sum = lax.optimization_barrier(jnp.sum(page_probs, axis=4))
    page_rounded = page_probs.astype(jnp.bfloat16).astype(jnp.float32)
    page_acc = jnp.einsum('pskgt,ptkd->pskgd', page_rounded, value_rows)
    denominator = jnp.einsum('rp,pskg->rskg', owned_f, page_sum, precision=EXACT)
    numerator = jnp.einsum('rp,pskgd->rskgd', owned_f, page_acc, precision=EXACT)
    fresh_probs = jnp.exp(fresh_scores - jnp.moveaxis(row_best, 1, 0)[..., None])
    denominator = denominator + jnp.moveaxis(lax.optimization_barrier(jnp.sum(fresh_probs, axis=4)), 0, 1)
    fresh_rounded = fresh_probs.astype(jnp.bfloat16).astype(jnp.float32)
    numerator = numerator + jnp.einsum('srkgu,urkd->rskgd', fresh_rounded, fresh_values)
    attended = numerator / denominator[..., None]
    attended = jnp.moveaxis(attended, 1, 0)
    return attended.reshape(step_count, req_count, head_count * head_width).astype(jnp.bfloat16)

def route_experts(normed, expert_ids, route_weights, gate_up, down_proj):
    row_total = STEPS * REQS
    blocks = expert_ids.reshape(STEPS, N_DP, REQ_DP, TOP)
    catalog = jnp.arange(EXPERTS, dtype=jnp.int32)
    named_mask = jnp.any(blocks[..., None] == catalog, axis=3).astype(jnp.int32)
    earlier = jnp.cumsum(named_mask, axis=2) - named_mask
    slot_rank = jnp.take_along_axis(earlier, blocks, axis=3)
    source = jnp.arange(N_DP, dtype=jnp.int32)[None, :, None, None]
    step_index = jnp.arange(STEPS, dtype=jnp.int32)[:, None, None, None]
    slot_keys = ((blocks * N_DP + source) * STEPS + step_index) * CAP + slot_rank
    row_index = (step_index * N_DP + source) * REQ_DP + jnp.arange(REQ_DP, dtype=jnp.int32)[None, None, :, None]
    row_index = jnp.broadcast_to(row_index, slot_keys.shape).astype(jnp.int32)
    slot_count = EXPERTS * N_DP * STEPS * CAP
    slot_rows = jnp.full((slot_count,), row_total, jnp.int32).at[slot_keys.reshape(-1)].set(row_index.reshape(-1))
    padded = jnp.concatenate([normed, jnp.zeros((1, D), normed.dtype)], axis=0)
    gathered = padded[slot_rows].reshape(EXPERTS, N_DP * STEPS * CAP, D)

    def one_expert(operands):
        expert_rows, weights_pair, weights_down = operands
        gate = jnp.dot(expert_rows, weights_pair[0], preferred_element_type=jnp.float32)
        up_value = jnp.dot(expert_rows, weights_pair[1], preferred_element_type=jnp.float32)
        activated = (jax.nn.silu(gate) * up_value).astype(jnp.bfloat16)
        return jnp.dot(activated, weights_down, preferred_element_type=jnp.float32).astype(jnp.bfloat16)
    results = lax.map(one_expert, (gathered, gate_up, down_proj)).reshape(slot_count, D)
    picked = results[slot_keys].astype(jnp.float32)
    share = route_weights.reshape(STEPS, N_DP, REQ_DP, TOP)
    share = share / lax.optimization_barrier(jnp.sum(share, axis=3, keepdims=True))
    mixture = lax.optimization_barrier(jnp.sum(share[..., None] * picked, axis=3))
    return mixture.reshape(row_total, D)

def reference(queries, fresh_kv, kv_pool, page_table, context_lengths, residual, out_weight, norm_gain, expert_ids, route_weights, gate_up, down_proj):
    query_blocks = jnp.moveaxis(queries.reshape(STEPS, N_DP, REQ_DP, HQ, HD), 1, 0)
    fresh_blocks = jnp.moveaxis(fresh_kv.reshape(STEPS, N_DP, REQ_DP, KVH, 2 * HD), 1, 0)
    pool_blocks = kv_pool.reshape(N_DP, POOL, PAGE, KVH, 2 * HD)
    table_blocks = page_table.reshape(N_DP, REQ_DP, MAXP)
    length_blocks = context_lengths.reshape(N_DP, REQ_DP)

    def per_block(operands):
        return attend(operands[0], operands[1], operands[2], operands[3], operands[4])
    attended = lax.map(per_block, (query_blocks, fresh_blocks, pool_blocks, table_blocks, length_blocks))
    attended = jnp.moveaxis(attended, 0, 1).reshape(STEPS * REQS, HQ * HD)
    projected = jnp.dot(attended, out_weight, preferred_element_type=jnp.float32)
    stream = residual.astype(jnp.float32).reshape(STEPS * REQS, D) + projected
    inverse = lax.rsqrt(lax.optimization_barrier(jnp.mean(stream * stream, axis=1)) + EPS)
    normed = (stream * inverse[:, None] * norm_gain[None, :]).astype(jnp.bfloat16)
    mixture = route_experts(normed, expert_ids, route_weights, gate_up, down_proj)
    return (stream + mixture).reshape(STEPS, REQS, D).astype(jnp.bfloat16)
```

```python
import functools
import math

import jax
import jax.numpy as jnp
from jax import lax
from jax.experimental import pallas as pl
from jax.experimental.pallas import tpu as pltpu
from jax.sharding import PartitionSpec as P

NEG = -1e30
EPS = 1e-06
EXACT = lax.Precision.HIGHEST
MESH = pl.DeviceIdType.MESH


def in_blocks(array, dim, length):
    before, after = (array.shape[:dim], array.shape[dim + 1 :])
    return jnp.moveaxis(array.reshape(*before, length, -1, *after), dim, 0)


def summed_on_arrival(array, axis, dim):
    length = lax.axis_size(axis)
    pieces = lax.all_to_all(in_blocks(array, dim, length), axis, 0, 0, tiled=True)
    return jnp.sum(pieces.astype(jnp.float32), axis=0)


def page_owners(table, lengths, pool_pages, page_len):
    pages = jnp.arange(pool_pages, dtype=jnp.int32)
    matches = table[:, :, None] == pages[None, None, :]
    ownership = jnp.any(matches, axis=1)
    slot_index = jnp.arange(table.shape[1], dtype=jnp.int32)
    position = jnp.sum(jnp.where(matches, slot_index[None, :, None], 0), axis=(0, 1))
    owner_length = jnp.sum(jnp.where(ownership, lengths[:, None], 0), axis=0)
    live_count = jnp.clip(owner_length - position * page_len, 0, page_len)
    return (ownership, live_count)


def attend(query_block, fresh_block, pool_block, table_block, length_block):
    step_count, req_count, head_count, head_width = query_block.shape
    pool_pages, page_len, kv_heads, _ = pool_block.shape
    group_size = head_count // kv_heads
    score_scale = 1.0 / math.sqrt(head_width)
    ownership, live_count = page_owners(table_block, length_block, pool_pages, page_len)
    owned_f = ownership.astype(jnp.float32)
    grouped = query_block.reshape(step_count, req_count, kv_heads, group_size, head_width)
    page_query = jnp.einsum(
        "rp,srkgd->pskgd",
        ownership.astype(jnp.bfloat16),
        grouped,
        preferred_element_type=jnp.float32,
    ).astype(jnp.bfloat16)
    key_rows = pool_block[..., :head_width]
    value_rows = pool_block[..., head_width:]
    page_scores = (
        jnp.einsum("pskgd,ptkd->pskgt", page_query, key_rows, preferred_element_type=jnp.float32)
        * score_scale
    )
    in_page = jnp.arange(page_len)[None, :] < live_count[:, None]
    page_scores = jnp.where(in_page[:, None, None, None, :], page_scores, NEG)
    fresh_keys = fresh_block[..., :head_width]
    fresh_values = fresh_block[..., head_width:]
    fresh_scores = (
        jnp.einsum("srkgd,urkd->srkgu", grouped, fresh_keys, preferred_element_type=jnp.float32)
        * score_scale
    )
    causal = jnp.arange(step_count)[:, None] >= jnp.arange(step_count)[None, :]
    fresh_scores = jnp.where(causal[:, None, None, None, :], fresh_scores, NEG)
    page_best = jnp.max(page_scores, axis=4)
    row_best = jnp.max(jnp.where(ownership[:, :, None, None, None], page_best[None], NEG), axis=1)
    row_best = jnp.maximum(row_best, jnp.moveaxis(jnp.max(fresh_scores, axis=4), 0, 1))
    owner_best = jnp.einsum("rp,rskg->pskg", owned_f, row_best, precision=EXACT)
    page_probs = jnp.exp(page_scores - owner_best[..., None])
    page_sum = jnp.sum(page_probs, axis=4)
    page_acc = jnp.einsum(
        "pskgt,ptkd->pskgd",
        page_probs.astype(jnp.bfloat16),
        value_rows,
        preferred_element_type=jnp.float32,
    )
    denominator = jnp.einsum("rp,pskg->rskg", owned_f, page_sum, precision=EXACT)
    numerator = jnp.einsum("rp,pskgd->rskgd", owned_f, page_acc, precision=EXACT)
    fresh_probs = jnp.exp(fresh_scores - jnp.moveaxis(row_best, 1, 0)[..., None])
    denominator = denominator + jnp.moveaxis(jnp.sum(fresh_probs, axis=4), 0, 1)
    numerator = numerator + jnp.einsum(
        "srkgu,urkd->rskgd",
        fresh_probs.astype(jnp.bfloat16),
        fresh_values,
        preferred_element_type=jnp.float32,
    )
    attended = jnp.moveaxis(numerator / denominator[..., None], 1, 0)
    return attended.reshape(step_count, req_count, head_count * head_width).astype(jnp.bfloat16)


def rcopy(src, dst, send_sem, recv_sem, axis, target):
    return pltpu.make_async_remote_copy(
        src_ref=src,
        dst_ref=dst,
        send_sem=send_sem,
        recv_sem=recv_sem,
        device_id={axis: target},
        device_id_type=MESH,
    )


def expert_kernel(
    n_dp,
    n_x,
    slots,
    block_ref,
    gate_up_hbm,
    down_hbm,
    out_ref,
    gath,
    gate_up,
    down,
    mix_t,
    rank_t,
    pick,
    slot_share,
    part,
    own,
    in_opp,
    in_left,
    in_right,
    act,
    contrib,
    mate_in,
    sum_r,
    sum_l,
    ring_r,
    ring_l,
    w_sem,
    ag_rs,
    ag_rr,
    ag_ls,
    ag_lr,
    ag_ms,
    ag_mr,
    x_s,
    x_r,
    a_s,
    a_r,
    m_s,
    m_r,
    rs_rs,
    rs_rr,
    rs_ls,
    rs_lr,
):
    width = out_ref.shape[1]
    hidden = act.shape[3]
    locals_ = gate_up.shape[0]
    rows = block_ref.shape[0]
    half = rows // 2
    chips = n_dp // 2
    steps_r, steps_l = chips // 2, chips - 1 - chips // 2
    chunk_dp = n_dp // n_x
    chunk_rows = chunk_dp * rows
    d = lax.axis_index("dp")
    q = lax.axis_index("expert")
    z, c = d // 2, d % 2
    right, left, mate = (d + 2) % n_dp, (d + n_dp - 2) % n_dp, d + 1 - 2 * c
    xr, xl, xo = (q + 1) % n_x, (q + n_x - 1) % n_x, (q + 2) % n_x

    barrier = pltpu.get_barrier_semaphore()
    for axis, target in (("dp", right), ("dp", left), ("dp", mate), ("expert", xr), ("expert", xl)):
        pl.semaphore_signal(barrier, inc=1, device_id={axis: target}, device_id_type=MESH)

    weights = [
        pltpu.make_async_copy(gate_up_hbm, gate_up, w_sem.at[0]),
        pltpu.make_async_copy(down_hbm, down, w_sem.at[1]),
    ]
    for w in weights:
        w.start()
    gath[d] = block_ref[...]
    pl.semaphore_wait(barrier, 5)

    def piece(ref, h):
        return ref.at[pl.ds(h * half, half)]

    def hop(idx, s, h, to_right):
        send, recv, target = (ag_rs, ag_rr, right) if to_right else (ag_ls, ag_lr, left)
        view = piece(gath.at[idx], h)
        return rcopy(view, view, send.at[s, h], recv.at[s, h], "dp", target)

    def to_mate(idx, k, h):
        view = piece(gath.at[idx], h)
        return rcopy(view, view, ag_ms.at[k, h], ag_mr.at[k, h], "dp", mate)

    def first(h, send, recv, axis, target):
        return rcopy(piece(block_ref, h), piece(gath.at[d], h), send, recv, axis, target)

    firsts = []
    for h in range(2):
        firsts.append(first(h, ag_rs.at[0, h], ag_rr.at[0, h], "dp", right))
        firsts.append(first(h, ag_ls.at[0, h], ag_lr.at[0, h], "dp", left))
        firsts.append(first(h, ag_ms.at[0, h], ag_mr.at[0, h], "dp", mate))
    for f in firsts:
        f.start()

    def from_left(s):
        return (d + n_dp - 2 * s) % n_dp

    def from_right(s):
        return (d + 2 * s) % n_dp

    def ag_step(s, carry):
        for h in range(2):
            hop(from_left(s), s - 1, h, True).wait_recv()
            hop(from_left(s), s, h, True).start()
            to_mate(from_left(s), s, h).start()
            hop(from_right(s), s - 1, h, False).wait_recv()

            @pl.when(s < steps_l)
            def _():
                hop(from_right(s), s, h, False).start()

            to_mate(from_right(s), steps_r + s, h).start()
        return carry

    lax.fori_loop(1, steps_r, ag_step, 0)
    for h in range(2):
        hop(from_left(steps_r), steps_r - 1, h, True).wait_recv()
        to_mate(from_left(steps_r), steps_r, h).start()

    def ag_drain(k, carry):
        for h in range(2):
            to_mate(d, k, h).wait()

            @pl.when(k < steps_r)
            def _():
                hop(d, k, h, True).wait_send()

            @pl.when(k < steps_l)
            def _():
                hop(d, k, h, False).wait_send()

        return carry

    lax.fori_loop(0, chips, ag_drain, 0)
    weights[0].wait()

    t_row = lax.broadcasted_iota(jnp.int32, (chunk_rows, chunk_rows), 0)
    t_col = lax.broadcasted_iota(jnp.int32, (chunk_rows, chunk_rows), 1)
    below = jnp.where(t_row < t_col, 1.0, 0.0).astype(jnp.bfloat16)
    slot_no = lax.broadcasted_iota(jnp.int32, (slots, chunk_rows), 0).astype(jnp.float32)
    experts = n_dp * locals_

    def project(r, keep):
        both = gath[pl.ds(r * chunk_dp, chunk_dp)]
        x = both[:, :, :width].reshape(chunk_rows, width)
        mix = both[:, :, width:].reshape(chunk_rows, both.shape[2] - width)
        mix_t[...] = jnp.transpose(mix.astype(jnp.float32))
        named = jnp.where(mix_t[...] > 0.0, 1.0, 0.0).astype(jnp.bfloat16)
        rank_t[...] = jnp.dot(named, below, preferred_element_type=jnp.float32)
        for l in range(locals_):
            e = d * locals_ + l
            share = mix_t[pl.ds(e, 1), :] + mix_t[pl.ds(experts + e, 1), :]
            hit = (rank_t[pl.ds(e, 1), :] == slot_no) & (share > 0.0)
            chosen = jnp.where(hit, 1.0, 0.0)
            at = pl.ds(l * slots, slots)
            pick[r, at, :] = chosen.astype(jnp.bfloat16)
            total = jnp.sum(chosen * share, axis=1, keepdims=True)
            slot_share[r, at, :] = jnp.broadcast_to(total, (slots, slot_share.shape[2]))
            picked = jnp.dot(
                chosen.astype(jnp.bfloat16), x, preferred_element_type=jnp.float32
            ).astype(jnp.bfloat16)
            for g in range(2):
                value = jnp.dot(picked, gate_up[l, g], preferred_element_type=jnp.float32)
                keep(at, pl.ds(g * hidden, hidden), value)

    def keep_part(r):
        def keep(at, columns, value):
            part[r, at, columns] = value.astype(jnp.bfloat16)

        return keep

    def keep_own(at, columns, value):
        own[at, columns] = value

    low, high = pl.ds(0, slots), pl.ds(slots, slots)

    def xsend(src, dst, k, target):
        return rcopy(src, dst, x_s.at[k], x_r.at[k], "expert", target)

    opp_a = xsend(part.at[xo, low], in_opp.at[0], 0, xr)
    opp_b = xsend(part.at[xo, high], in_opp.at[1], 1, xl)
    right_b = xsend(part.at[xr, high], in_left.at[high], 2, xr)
    left_a = xsend(part.at[xl, low], in_right.at[low], 3, xl)
    right_a = xsend(part.at[xr, low], in_left.at[low], 4, xr)
    left_b = xsend(part.at[xl, high], in_right.at[high], 5, xl)

    project(xo, keep_part(xo))
    opp_a.start()
    opp_b.start()
    project(xr, keep_part(xr))
    right_b.start()
    project(xl, keep_part(xl))
    left_a.start()
    project(q, keep_own)
    opp_a.wait_recv()
    part[xr, low, :] = (
        part[xr, low, :].astype(jnp.float32) + in_opp[0].astype(jnp.float32)
    ).astype(jnp.bfloat16)
    right_a.start()
    opp_b.wait_recv()
    part[xl, high, :] = (
        part[xl, high, :].astype(jnp.float32) + in_opp[1].astype(jnp.float32)
    ).astype(jnp.bfloat16)
    left_b.start()
    right_b.wait_recv()
    left_a.wait_recv()
    right_a.wait_recv()
    left_b.wait_recv()

    def asend(owner, part_no, k, target):
        view = act.at[owner, part_no]
        return rcopy(view, view, a_s.at[k], a_r.at[k], "expert", target)

    for l in range(2):
        at = pl.ds(l * slots, slots)
        total = own[at, :] + in_left[at, :].astype(jnp.float32) + in_right[at, :].astype(jnp.float32)
        gate, up = total[:, :hidden], total[:, hidden:]
        act[q, l] = (gate / (1.0 + jnp.exp(-gate)) * up).astype(jnp.bfloat16)
        if l == 0:
            asend(q, 0, 0, xr).start()
        else:
            asend(q, 1, 1, xl).start()
    asend(q, 1, 2, xr).start()
    asend(q, 0, 3, xl).start()
    weights[1].wait()

    def combine(r):
        scaled = []
        for l in range(locals_):
            value = jnp.dot(act[r, l], down[l], preferred_element_type=jnp.float32)
            scaled.append(value * slot_share[r, pl.ds(l * slots, slots), :1])
        rows_out = jnp.concatenate(scaled, axis=0).astype(jnp.bfloat16)
        mixed = lax.dot_general(
            pick[r], rows_out, (((0,), (0,)), ((), ())), preferred_element_type=jnp.float32
        ).astype(jnp.bfloat16)
        for k in range(chunk_dp):
            contrib[k % 2, r * (chunk_dp // 2) + k // 2] = mixed[k * rows : (k + 1) * rows]

    def mate_send(r):
        at = pl.ds(r * (chunk_dp // 2), chunk_dp // 2)
        return rcopy(contrib.at[1 - c, at], mate_in.at[at], m_s.at[r], m_r.at[r], "dp", mate)

    combine(q)
    mate_send(q).start()
    asend(xl, 0, 0, xr).wait_recv()
    asend(xl, 0, 4, xr).start()
    asend(xr, 1, 1, xl).wait_recv()
    asend(xr, 1, 5, xl).start()
    asend(xl, 1, 2, xr).wait_recv()
    combine(xl)
    mate_send(xl).start()
    asend(xr, 0, 3, xl).wait_recv()
    combine(xr)
    mate_send(xr).start()
    asend(xo, 0, 4, xr).wait_recv()
    asend(xo, 1, 5, xl).wait_recv()
    combine(xo)
    mate_send(xo).start()
    for r in (q, xl, xr, xo):
        mate_send(r).wait_recv()

    def ring(k, h, to_right):
        if to_right:
            return rcopy(
                piece(sum_r.at[k], h), piece(ring_r.at[k], h), rs_rs.at[k, h], rs_rr.at[k, h], "dp", right
            )
        return rcopy(
            piece(sum_l.at[k], h), piece(ring_l.at[k], h), rs_ls.at[k, h], rs_lr.at[k, h], "dp", left
        )

    def mine(chip, h):
        at = pl.ds(h * half, half)
        return contrib[c, chip, at].astype(jnp.float32) + mate_in[chip, at].astype(jnp.float32)

    far_r = (z + steps_r) % chips
    far_l = (z + chips - steps_l) % chips
    for h in range(2):
        at = pl.ds(h * half, half)
        sum_r[0, at] = mine(far_r, h).astype(jnp.bfloat16)
        ring(0, h, True).start()
        sum_l[0, at] = mine(far_l, h).astype(jnp.bfloat16)
        ring(0, h, False).start()

    def rs_step(k, carry):
        for h in range(2):
            at = pl.ds(h * half, half)
            ring(k - 1, h, True).wait_recv()
            value = mine((z + steps_r - k) % chips, h) + ring_r[k - 1, at].astype(jnp.float32)
            sum_r[k, at] = value.astype(jnp.bfloat16)
            ring(k, h, True).start()

            @pl.when(k < steps_l)
            def _():
                ring(k - 1, h, False).wait_recv()
                other = mine((z + chips - steps_l + k) % chips, h) + ring_l[k - 1, at].astype(jnp.float32)
                sum_l[k, at] = other.astype(jnp.bfloat16)
                ring(k, h, False).start()

        return carry

    lax.fori_loop(1, steps_r, rs_step, 0)
    for h in range(2):
        at = pl.ds(h * half, half)
        ring(steps_r - 1, h, True).wait_recv()
        ring(steps_l - 1, h, False).wait_recv()
        out_ref[at, :] = (
            mine(z, h)
            + ring_r[steps_r - 1, at].astype(jnp.float32)
            + ring_l[steps_l - 1, at].astype(jnp.float32)
        )

    for copy in (opp_a, opp_b, right_b, left_a, right_a, left_b):
        copy.wait_send()
    asend(q, 0, 0, xr).wait_send()
    asend(q, 1, 1, xl).wait_send()
    asend(q, 1, 2, xr).wait_send()
    asend(q, 0, 3, xl).wait_send()
    asend(xl, 0, 4, xr).wait_send()
    asend(xr, 1, 5, xl).wait_send()
    for r in (q, xl, xr, xo):
        mate_send(r).wait_send()

    def rs_drain(k, carry):
        for h in range(2):
            ring(k, h, True).wait_send()

            @pl.when(k < steps_l)
            def _():
                ring(k, h, False).wait_send()

        return carry

    lax.fori_loop(0, steps_r, rs_drain, 0)


def expert_layer(block, gate_up, down_proj, per_step, steps):
    n_dp, n_x = lax.axis_size("dp"), lax.axis_size("expert")
    rows = block.shape[0]
    locals_, _, width, hidden = gate_up.shape
    chips = n_dp // 2
    slots = (n_dp // n_x) * steps * per_step
    chunk_rows = (n_dp // n_x) * rows
    lanes = block.shape[1] - width
    half_r, half_l = chips // 2, chips - 1 - chips // 2
    bf16, f32, dma = jnp.bfloat16, jnp.float32, pltpu.SemaphoreType.DMA
    vmem = pl.BlockSpec(memory_space=pltpu.VMEM)
    anywhere = pl.BlockSpec(memory_space=pl.ANY)
    return pl.pallas_call(
        functools.partial(expert_kernel, n_dp, n_x, slots),
        out_shape=jax.ShapeDtypeStruct((rows, width), f32),
        in_specs=[vmem, anywhere, anywhere],
        out_specs=vmem,
        scratch_shapes=[
            pltpu.VMEM((n_dp, rows, width + lanes), bf16),
            pltpu.VMEM(gate_up.shape, bf16),
            pltpu.VMEM(down_proj.shape, bf16),
            pltpu.VMEM((lanes, chunk_rows), f32),
            pltpu.VMEM((lanes, chunk_rows), f32),
            pltpu.VMEM((n_x, locals_ * slots, chunk_rows), bf16),
            pltpu.VMEM((n_x, locals_ * slots, 128), f32),
            pltpu.VMEM((n_x, 2 * slots, 2 * hidden), bf16),
            pltpu.VMEM((2 * slots, 2 * hidden), f32),
            pltpu.VMEM((2, slots, 2 * hidden), bf16),
            pltpu.VMEM((2 * slots, 2 * hidden), bf16),
            pltpu.VMEM((2 * slots, 2 * hidden), bf16),
            pltpu.VMEM((n_x, 2, slots, hidden), bf16),
            pltpu.VMEM((2, chips, rows, width), bf16),
            pltpu.VMEM((chips, rows, width), bf16),
            pltpu.VMEM((half_r, rows, width), bf16),
            pltpu.VMEM((half_l, rows, width), bf16),
            pltpu.VMEM((half_r, rows, width), bf16),
            pltpu.VMEM((half_l, rows, width), bf16),
            dma((2,)),
            dma((half_r, 2)),
            dma((half_r, 2)),
            dma((half_l, 2)),
            dma((half_l, 2)),
            dma((chips, 2)),
            dma((chips, 2)),
            dma((6,)),
            dma((6,)),
            dma((6,)),
            dma((6,)),
            dma((n_x,)),
            dma((n_x,)),
            dma((half_r, 2)),
            dma((half_r, 2)),
            dma((half_l, 2)),
            dma((half_l, 2)),
        ],
        compiler_params=pltpu.CompilerParams(
            collective_id=0, has_side_effects=True, vmem_limit_bytes=56 * 1024 * 1024
        ),
    )(block, gate_up, down_proj)


def mix_columns(expert_ids, route_weights, expert_total):
    share = route_weights / jnp.sum(route_weights, axis=2, keepdims=True)
    catalog = jnp.arange(expert_total, dtype=jnp.int32)
    dense = jnp.sum(jnp.where(expert_ids[..., None] == catalog, share[..., None], 0.0), axis=2)
    dense = dense.reshape(-1, expert_total)
    top = dense.astype(jnp.bfloat16)
    rest = (dense - top.astype(jnp.float32)).astype(jnp.bfloat16)
    return jnp.concatenate([top, rest], axis=1)


def body(
    queries,
    fresh_kv,
    kv_pool,
    page_table,
    context_lengths,
    residual,
    out_weight,
    norm_gain,
    expert_ids,
    route_weights,
    gate_up,
    down_proj,
):
    attended = attend(queries, fresh_kv, kv_pool, page_table, context_lengths)
    step_count, req_count, head_cols = attended.shape
    flat_attended = attended.reshape(step_count * req_count, head_cols)
    partial_out = jnp.dot(
        flat_attended,
        lax.all_gather(out_weight, "dp", axis=1, tiled=True),
        preferred_element_type=jnp.float32,
    )
    projected = summed_on_arrival(partial_out.astype(jnp.bfloat16), "expert", 1)
    quarter = projected.shape[1]
    stream = residual.astype(jnp.float32).reshape(step_count * req_count, quarter) + projected
    squares = lax.psum(jnp.sum(stream * stream, axis=1), "expert")
    model_width = quarter * lax.axis_size("expert")
    inverse = lax.rsqrt(squares / model_width + EPS)
    normed = (stream * inverse[:, None] * norm_gain[None, :]).astype(jnp.bfloat16)
    dp_count = lax.axis_size("dp")
    local_experts = gate_up.shape[0]
    expert_total = local_experts * dp_count
    top_count = expert_ids.shape[2]
    capacity = min(
        req_count, max(2, (5 * req_count * top_count + 2 * expert_total - 1) // (2 * expert_total))
    )
    block = jnp.concatenate([normed, mix_columns(expert_ids, route_weights, expert_total)], axis=1)
    mixture = expert_layer(block, gate_up, down_proj, capacity, step_count)
    return (stream + mixture).reshape(step_count, req_count, quarter).astype(jnp.bfloat16)


def solution(mesh):
    return jax.shard_map(
        body,
        mesh=mesh,
        in_specs=(
            P(None, ("groups", "dp"), "expert", None),
            P(None, ("groups", "dp"), "expert", None),
            P(("groups", "dp"), None, "expert", None),
            P(("groups", "dp"), None),
            P(("groups", "dp")),
            P(None, ("groups", "dp"), "expert"),
            P("expert", "dp"),
            P("expert"),
            P(None, ("groups", "dp"), None),
            P(None, ("groups", "dp"), None),
            P("dp", None, "expert", None),
            P("dp", None, "expert"),
        ),
        out_specs=P(None, ("groups", "dp"), "expert"),
        check_vma=False,
    )
```

```python
import functools
import math

import jax
import jax.numpy as jnp
from jax import lax
from jax.experimental import pallas as pl
from jax.experimental.pallas import tpu as pltpu
from jax.sharding import PartitionSpec as P

NEG = -1e30
EPS = 1e-06
EXACT = lax.Precision.HIGHEST
MESH = pl.DeviceIdType.MESH


def page_owners(table, lengths, pool_pages, page_len):
    pages = jnp.arange(pool_pages, dtype=jnp.int32)
    matches = table[:, :, None] == pages[None, None, :]
    ownership = jnp.any(matches, axis=1)
    slot_index = jnp.arange(table.shape[1], dtype=jnp.int32)
    position = jnp.sum(jnp.where(matches, slot_index[None, :, None], 0), axis=(0, 1))
    owner_length = jnp.sum(jnp.where(ownership, lengths[:, None], 0), axis=0)
    live_count = jnp.clip(owner_length - position * page_len, 0, page_len)
    return (ownership, live_count)


def attend(query_block, fresh_block, pool_block, table_block, length_block):
    step_count, req_count, head_count, head_width = query_block.shape
    pool_pages, page_len, kv_heads, _ = pool_block.shape
    group_size = head_count // kv_heads
    score_scale = 1.0 / math.sqrt(head_width)
    ownership, live_count = page_owners(table_block, length_block, pool_pages, page_len)
    owned_f = ownership.astype(jnp.float32)
    grouped = query_block.reshape(step_count, req_count, kv_heads, group_size, head_width)
    page_query = jnp.einsum(
        "rp,srkgd->pskgd",
        ownership.astype(jnp.bfloat16),
        grouped,
        preferred_element_type=jnp.float32,
    ).astype(jnp.bfloat16)
    key_rows = pool_block[..., :head_width]
    value_rows = pool_block[..., head_width:]
    page_scores = (
        jnp.einsum("pskgd,ptkd->pskgt", page_query, key_rows, preferred_element_type=jnp.float32)
        * score_scale
    )
    in_page = jnp.arange(page_len)[None, :] < live_count[:, None]
    page_scores = jnp.where(in_page[:, None, None, None, :], page_scores, NEG)
    fresh_keys = fresh_block[..., :head_width]
    fresh_values = fresh_block[..., head_width:]
    fresh_scores = (
        jnp.einsum("srkgd,urkd->srkgu", grouped, fresh_keys, preferred_element_type=jnp.float32)
        * score_scale
    )
    causal = jnp.arange(step_count)[:, None] >= jnp.arange(step_count)[None, :]
    fresh_scores = jnp.where(causal[:, None, None, None, :], fresh_scores, NEG)
    page_best = jnp.max(page_scores, axis=4)
    row_best = jnp.max(jnp.where(ownership[:, :, None, None, None], page_best[None], NEG), axis=1)
    row_best = jnp.maximum(row_best, jnp.moveaxis(jnp.max(fresh_scores, axis=4), 0, 1))
    owner_best = jnp.einsum("rp,rskg->pskg", owned_f, row_best, precision=EXACT)
    page_probs = jnp.exp(page_scores - owner_best[..., None])
    page_sum = jnp.sum(page_probs, axis=4)
    page_acc = jnp.einsum(
        "pskgt,ptkd->pskgd",
        page_probs.astype(jnp.bfloat16),
        value_rows,
        preferred_element_type=jnp.float32,
    )
    denominator = jnp.einsum("rp,pskg->rskg", owned_f, page_sum, precision=EXACT)
    numerator = jnp.einsum("rp,pskgd->rskgd", owned_f, page_acc, precision=EXACT)
    fresh_probs = jnp.exp(fresh_scores - jnp.moveaxis(row_best, 1, 0)[..., None])
    denominator = denominator + jnp.moveaxis(jnp.sum(fresh_probs, axis=4), 0, 1)
    numerator = numerator + jnp.einsum(
        "srkgu,urkd->rskgd",
        fresh_probs.astype(jnp.bfloat16),
        fresh_values,
        preferred_element_type=jnp.float32,
    )
    attended = jnp.moveaxis(numerator / denominator[..., None], 1, 0)
    return attended.reshape(step_count, req_count, head_count * head_width).astype(jnp.bfloat16)


def rcopy(src, dst, send_sem, recv_sem, axis, target):
    return pltpu.make_async_remote_copy(
        src_ref=src,
        dst_ref=dst,
        send_sem=send_sem,
        recv_sem=recv_sem,
        device_id={axis: target},
        device_id_type=MESH,
    )


def layer_kernel(
    n_dp,
    n_x,
    slots,
    attended_ref,
    residual_ref,
    gain_ref,
    out_weight_ref,
    gate_up_hbm,
    down_hbm,
    out_ref,
    heads,
    product,
    back,
    heads_in,
    squares,
    stream,
    own_rows,
    gath,
    gate_up,
    down,
    mix_t,
    rank_t,
    pick,
    slot_share,
    part,
    own,
    in_opp,
    in_left,
    in_right,
    act,
    contrib,
    mate_in,
    sum_r,
    sum_l,
    ring_r,
    ring_l,
    w_sem,
    back_s,
    back_r,
    h_s,
    h_r,
    q_s,
    q_r,
    x_s,
    x_r,
    a_s,
    a_r,
    m_s,
    m_r,
    rs_rs,
    rs_rr,
    rs_ls,
    rs_lr,
    *gather_sems,
):
    rows, width = out_ref.shape
    hidden = act.shape[3]
    locals_ = gate_up.shape[0]
    half = rows // 2
    chips = n_dp // 2
    steps_r, steps_l = chips // 2, chips - 1 - chips // 2
    chunk_dp = n_dp // n_x
    chunk_rows = chunk_dp * rows
    head_cols = out_weight_ref.shape[0]
    columns = out_weight_ref.shape[1]
    d = lax.axis_index("dp")
    q = lax.axis_index("expert")
    z, c = d // 2, d % 2
    right, left, mate = (d + 2) % n_dp, (d + n_dp - 2) % n_dp, d + 1 - 2 * c
    xr, xl, xo = (q + 1) % n_x, (q + n_x - 1) % n_x, (q + 2) % n_x

    barrier = pltpu.get_barrier_semaphore()
    neighbours = (("dp", right), ("dp", left), ("dp", mate), ("expert", xr), ("expert", xl), ("expert", xo))
    for axis, target in neighbours:
        pl.semaphore_signal(barrier, inc=1, device_id={axis: target}, device_id_type=MESH)

    weights = [
        pltpu.make_async_copy(gate_up_hbm, gate_up, w_sem.at[0]),
        pltpu.make_async_copy(down_hbm, down, w_sem.at[1]),
    ]
    for w in weights:
        w.start()
    pl.semaphore_wait(barrier, len(neighbours))

    def piece(ref, h):
        return ref.at[pl.ds(h * half, half)]

    def from_left(s):
        return (d + n_dp - 2 * s) % n_dp

    def from_right(s):
        return (d + 2 * s) % n_dp

    def mate_left(s):
        return (mate + n_dp - 2 * s) % n_dp

    def mate_right(s):
        return (mate + 2 * s) % n_dp

    class Gather:
        def __init__(self, source, buffer, sems):
            self.source, self.buffer = source, buffer
            self.rs, self.rr, self.ls, self.lr, self.ms, self.mr = sems

        def hop(self, idx, s, h, to_right):
            send, recv, target = (self.rs, self.rr, right) if to_right else (self.ls, self.lr, left)
            view = piece(self.buffer.at[idx], h)
            return rcopy(view, view, send.at[s, h], recv.at[s, h], "dp", target)

        def to_mate(self, idx, k, h):
            view = piece(self.buffer.at[idx], h)
            return rcopy(view, view, self.ms.at[k, h], self.mr.at[k, h], "dp", mate)

        def begin(self):
            for h in range(2):
                src, dst = piece(self.source, h), piece(self.buffer.at[d], h)
                rcopy(src, dst, self.rs.at[0, h], self.rr.at[0, h], "dp", right).start()
                rcopy(src, dst, self.ls.at[0, h], self.lr.at[0, h], "dp", left).start()
                rcopy(src, dst, self.ms.at[0, h], self.mr.at[0, h], "dp", mate).start()
            self.buffer[d] = self.source[...]

        def step(self, s):
            for h in range(2):
                self.hop(from_left(s), s - 1, h, True).wait_recv()
                self.hop(from_left(s), s, h, True).start()
                self.to_mate(from_left(s), s, h).start()
                self.hop(from_right(s), s - 1, h, False).wait_recv()

                @pl.when(s < steps_l)
                def _():
                    self.hop(from_right(s), s, h, False).start()

                self.to_mate(from_right(s), steps_r + s, h).start()

        def last(self):
            for h in range(2):
                self.hop(from_left(steps_r), steps_r - 1, h, True).wait_recv()
                self.to_mate(from_left(steps_r), steps_r, h).start()

        def await_mate(self, k):
            for h in range(2):
                self.to_mate(d, k, h).wait_recv()

        def drain(self):
            def one(k, carry):
                for h in range(2):
                    self.to_mate(d, k, h).wait_send()

                    @pl.when(k < steps_r)
                    def _():
                        self.hop(d, k, h, True).wait_send()

                    @pl.when(k < steps_l)
                    def _():
                        self.hop(d, k, h, False).wait_send()

                return carry

            lax.fori_loop(0, chips, one, 0)

    first = Gather(attended_ref, heads, gather_sems[:6])
    second = Gather(own_rows, gath, gather_sems[6:])

    def give_back(idx):
        return rcopy(product.at[idx], back.at[d], back_s.at[idx], back_r.at[d], "dp", idx)

    def multiply(blocks):
        x = jnp.concatenate([heads[b][:, :head_cols] for b in blocks], axis=0)
        y = jnp.dot(x, out_weight_ref[...], preferred_element_type=jnp.float32).astype(jnp.bfloat16)
        for k, b in enumerate(blocks):
            product[b] = y[k * rows : (k + 1) * rows]

    first.begin()

    def heads_step(s, carry):
        first.step(s)
        first.await_mate(s - 1)

        @pl.when(s > 1)
        def _():
            first.await_mate(steps_r + s - 1)

        multiply([from_left(s), from_right(s), mate_left(s - 1), mate_right(s - 1)])
        give_back(from_left(s)).start()
        give_back(from_right(s)).start()
        give_back(mate_left(s - 1)).start()

        @pl.when(s > 1)
        def _():
            give_back(mate_right(s - 1)).start()

        return carry

    lax.fori_loop(1, steps_r, heads_step, 0)
    first.last()
    first.await_mate(steps_l)
    first.await_mate(steps_r + steps_l)
    multiply([from_left(steps_r), mate_left(steps_l), mate_right(steps_l), d])
    give_back(from_left(steps_r)).start()
    give_back(mate_left(steps_l)).start()
    give_back(mate_right(steps_l)).start()
    back[d] = product[d]
    first.await_mate(steps_r)
    multiply([mate_left(steps_r)])
    give_back(mate_left(steps_r)).start()

    t_row = lax.broadcasted_iota(jnp.int32, (chunk_rows, chunk_rows), 0)
    t_col = lax.broadcasted_iota(jnp.int32, (chunk_rows, chunk_rows), 1)
    below = jnp.where(t_row < t_col, 1.0, 0.0).astype(jnp.bfloat16)
    slot_no = lax.broadcasted_iota(jnp.int32, (slots, chunk_rows), 0).astype(jnp.float32)
    experts = n_dp * locals_

    def prepare(r, carry):
        both = heads[pl.ds(r * chunk_dp, chunk_dp)]
        mix = both[:, :, head_cols:].reshape(chunk_rows, heads.shape[2] - head_cols)
        mix_t[...] = jnp.transpose(mix.astype(jnp.float32))
        named = jnp.where(mix_t[...] > 0.0, 1.0, 0.0).astype(jnp.bfloat16)
        rank_t[...] = jnp.dot(named, below, preferred_element_type=jnp.float32)
        for l in range(locals_):
            e = d * locals_ + l
            share = mix_t[pl.ds(e, 1), :] + mix_t[pl.ds(experts + e, 1), :]
            hit = (rank_t[pl.ds(e, 1), :] == slot_no) & (share > 0.0)
            chosen = jnp.where(hit, 1.0, 0.0)
            at = pl.ds(l * slots, slots)
            pick[r, at, :] = chosen.astype(jnp.bfloat16)
            total = jnp.sum(chosen * share, axis=1, keepdims=True)
            slot_share[r, at, :] = jnp.broadcast_to(total, (slots, slot_share.shape[2]))
        return carry

    lax.fori_loop(0, n_x, prepare, 0)

    def await_back(o, carry):
        j = (d + o) % n_dp
        rcopy(product.at[j], back.at[j], back_s.at[j], back_r.at[j], "dp", j).wait_recv()
        return carry

    lax.fori_loop(1, n_dp, await_back, 0)

    def heads_send(k, target):
        src = back.at[pl.ds(target * chunk_dp, chunk_dp)]
        return rcopy(src, heads_in.at[k], h_s.at[k], h_r.at[k], "expert", target)

    def squares_send(k, target):
        return rcopy(squares.at[0], squares.at[k + 1], q_s.at[k], q_r.at[k], "expert", target)

    peers = (xo, xr, xl)
    for k, target in enumerate(peers):
        heads_send(k, target).start()
    for k, target in enumerate(peers):
        heads_send(k, target).wait_recv()
    square = jnp.zeros((rows, 1), jnp.float32)
    for k in range(chunk_dp):
        at = pl.ds(k * columns, columns)
        value = residual_ref[:, at].astype(jnp.float32) + back[q * chunk_dp + k].astype(jnp.float32)
        for p in range(len(peers)):
            value = value + heads_in[p, k].astype(jnp.float32)
        stream[:, at] = value
        square = square + jnp.sum(value * value, axis=1, keepdims=True)
    squares[0] = jnp.broadcast_to(square, squares.shape[1:])
    for k, target in enumerate(peers):
        squares_send(k, target).start()
    for k, target in enumerate(peers):
        squares_send(k, target).wait_recv()
    whole = squares[0] + squares[1] + squares[2] + squares[3]
    inverse = lax.rsqrt(whole[:, :1] / (width * n_x) + EPS)
    own_rows[...] = (stream[...] * inverse * gain_ref[...]).astype(jnp.bfloat16)

    second.begin()

    def rows_step(s, carry):
        second.step(s)
        return carry

    lax.fori_loop(1, steps_r, rows_step, 0)
    second.last()

    def rows_mate(k, carry):
        second.await_mate(k)
        return carry

    lax.fori_loop(0, chips, rows_mate, 0)
    weights[0].wait()

    def project(r, keep):
        x = gath[pl.ds(r * chunk_dp, chunk_dp)].reshape(chunk_rows, width)
        for l in range(locals_):
            at = pl.ds(l * slots, slots)
            picked = jnp.dot(pick[r, at, :], x, preferred_element_type=jnp.float32).astype(jnp.bfloat16)
            for g in range(2):
                value = jnp.dot(picked, gate_up[l, g], preferred_element_type=jnp.float32)
                keep(at, pl.ds(g * hidden, hidden), value)

    def keep_part(r):
        def keep(at, columns, value):
            part[r, at, columns] = value.astype(jnp.bfloat16)

        return keep

    def keep_own(at, columns, value):
        own[at, columns] = value

    low, high = pl.ds(0, slots), pl.ds(slots, slots)

    def xsend(src, dst, k, target):
        return rcopy(src, dst, x_s.at[k], x_r.at[k], "expert", target)

    opp_a = xsend(part.at[xo, low], in_opp.at[0], 0, xr)
    opp_b = xsend(part.at[xo, high], in_opp.at[1], 1, xl)
    right_b = xsend(part.at[xr, high], in_left.at[high], 2, xr)
    left_a = xsend(part.at[xl, low], in_right.at[low], 3, xl)
    right_a = xsend(part.at[xr, low], in_left.at[low], 4, xr)
    left_b = xsend(part.at[xl, high], in_right.at[high], 5, xl)

    project(xo, keep_part(xo))
    opp_a.start()
    opp_b.start()
    project(xr, keep_part(xr))
    right_b.start()
    project(xl, keep_part(xl))
    left_a.start()
    project(q, keep_own)
    opp_a.wait_recv()
    part[xr, low, :] = (
        part[xr, low, :].astype(jnp.float32) + in_opp[0].astype(jnp.float32)
    ).astype(jnp.bfloat16)
    right_a.start()
    opp_b.wait_recv()
    part[xl, high, :] = (
        part[xl, high, :].astype(jnp.float32) + in_opp[1].astype(jnp.float32)
    ).astype(jnp.bfloat16)
    left_b.start()
    right_b.wait_recv()
    left_a.wait_recv()
    right_a.wait_recv()
    left_b.wait_recv()

    def asend(owner, part_no, k, target):
        view = act.at[owner, part_no]
        return rcopy(view, view, a_s.at[k], a_r.at[k], "expert", target)

    for l in range(2):
        at = pl.ds(l * slots, slots)
        total = own[at, :] + in_left[at, :].astype(jnp.float32) + in_right[at, :].astype(jnp.float32)
        gate, up = total[:, :hidden], total[:, hidden:]
        act[q, l] = (gate / (1.0 + jnp.exp(-gate)) * up).astype(jnp.bfloat16)
        if l == 0:
            asend(q, 0, 0, xr).start()
        else:
            asend(q, 1, 1, xl).start()
    asend(q, 1, 2, xr).start()
    asend(q, 0, 3, xl).start()
    weights[1].wait()

    def combine(r):
        scaled = []
        for l in range(locals_):
            value = jnp.dot(act[r, l], down[l], preferred_element_type=jnp.float32)
            scaled.append(value * slot_share[r, pl.ds(l * slots, slots), :1])
        rows_out = jnp.concatenate(scaled, axis=0).astype(jnp.bfloat16)
        mixed = lax.dot_general(
            pick[r], rows_out, (((0,), (0,)), ((), ())), preferred_element_type=jnp.float32
        ).astype(jnp.bfloat16)
        for k in range(chunk_dp):
            contrib[k % 2, r * (chunk_dp // 2) + k // 2] = mixed[k * rows : (k + 1) * rows]

    def mate_send(r):
        at = pl.ds(r * (chunk_dp // 2), chunk_dp // 2)
        return rcopy(contrib.at[1 - c, at], mate_in.at[at], m_s.at[r], m_r.at[r], "dp", mate)

    combine(q)
    mate_send(q).start()
    asend(xl, 0, 0, xr).wait_recv()
    asend(xl, 0, 4, xr).start()
    asend(xr, 1, 1, xl).wait_recv()
    asend(xr, 1, 5, xl).start()
    asend(xl, 1, 2, xr).wait_recv()
    combine(xl)
    mate_send(xl).start()
    asend(xr, 0, 3, xl).wait_recv()
    combine(xr)
    mate_send(xr).start()
    asend(xo, 0, 4, xr).wait_recv()
    asend(xo, 1, 5, xl).wait_recv()
    combine(xo)
    mate_send(xo).start()
    for r in (q, xl, xr, xo):
        mate_send(r).wait_recv()

    def ring(k, h, to_right):
        if to_right:
            return rcopy(
                piece(sum_r.at[k], h), piece(ring_r.at[k], h), rs_rs.at[k, h], rs_rr.at[k, h], "dp", right
            )
        return rcopy(
            piece(sum_l.at[k], h), piece(ring_l.at[k], h), rs_ls.at[k, h], rs_lr.at[k, h], "dp", left
        )

    def mine(chip, h):
        at = pl.ds(h * half, half)
        return contrib[c, chip, at].astype(jnp.float32) + mate_in[chip, at].astype(jnp.float32)

    far_r = (z + steps_r) % chips
    far_l = (z + chips - steps_l) % chips
    for h in range(2):
        at = pl.ds(h * half, half)
        sum_r[0, at] = mine(far_r, h).astype(jnp.bfloat16)
        ring(0, h, True).start()
        sum_l[0, at] = mine(far_l, h).astype(jnp.bfloat16)
        ring(0, h, False).start()

    def rs_step(k, carry):
        for h in range(2):
            at = pl.ds(h * half, half)
            ring(k - 1, h, True).wait_recv()
            value = mine((z + steps_r - k) % chips, h) + ring_r[k - 1, at].astype(jnp.float32)
            sum_r[k, at] = value.astype(jnp.bfloat16)
            ring(k, h, True).start()

            @pl.when(k < steps_l)
            def _():
                ring(k - 1, h, False).wait_recv()
                other = mine((z + chips - steps_l + k) % chips, h) + ring_l[k - 1, at].astype(jnp.float32)
                sum_l[k, at] = other.astype(jnp.bfloat16)
                ring(k, h, False).start()

        return carry

    lax.fori_loop(1, steps_r, rs_step, 0)
    for h in range(2):
        at = pl.ds(h * half, half)
        ring(steps_r - 1, h, True).wait_recv()
        ring(steps_l - 1, h, False).wait_recv()
        out_ref[at, :] = (
            stream[at, :]
            + mine(z, h)
            + ring_r[steps_r - 1, at].astype(jnp.float32)
            + ring_l[steps_l - 1, at].astype(jnp.float32)
        )

    first.drain()
    second.drain()
    for k, target in enumerate(peers):
        heads_send(k, target).wait_send()
        squares_send(k, target).wait_send()

    def back_drain(o, carry):
        give_back((d + o) % n_dp).wait_send()
        return carry

    lax.fori_loop(1, n_dp, back_drain, 0)
    for copy in (opp_a, opp_b, right_b, left_a, right_a, left_b):
        copy.wait_send()
    asend(q, 0, 0, xr).wait_send()
    asend(q, 1, 1, xl).wait_send()
    asend(q, 1, 2, xr).wait_send()
    asend(q, 0, 3, xl).wait_send()
    asend(xl, 0, 4, xr).wait_send()
    asend(xr, 1, 5, xl).wait_send()
    for r in (q, xl, xr, xo):
        mate_send(r).wait_send()

    def rs_drain(k, carry):
        for h in range(2):
            ring(k, h, True).wait_send()

            @pl.when(k < steps_l)
            def _():
                ring(k, h, False).wait_send()

        return carry

    lax.fori_loop(0, steps_r, rs_drain, 0)


def layer(attended, residual, gain, out_weight, gate_up, down_proj, per_step, steps):
    n_dp, n_x = lax.axis_size("dp"), lax.axis_size("expert")
    rows = attended.shape[0]
    locals_, _, width, hidden = gate_up.shape
    head_cols, columns = out_weight.shape
    chips = n_dp // 2
    chunk_dp = n_dp // n_x
    slots = chunk_dp * steps * per_step
    chunk_rows = chunk_dp * rows
    lanes = attended.shape[1] - head_cols
    half_r, half_l = chips // 2, chips - 1 - chips // 2
    bf16, f32, dma = jnp.bfloat16, jnp.float32, pltpu.SemaphoreType.DMA
    vmem = pl.BlockSpec(memory_space=pltpu.VMEM)
    anywhere = pl.BlockSpec(memory_space=pl.ANY)
    gather_sems = [dma((n, 2)) for n in (half_r, half_r, half_l, half_l, chips, chips)]
    return pl.pallas_call(
        functools.partial(layer_kernel, n_dp, n_x, slots),
        out_shape=jax.ShapeDtypeStruct((rows, width), f32),
        in_specs=[vmem, vmem, vmem, vmem, anywhere, anywhere],
        out_specs=vmem,
        scratch_shapes=[
            pltpu.VMEM((n_dp, rows, head_cols + lanes), bf16),
            pltpu.VMEM((n_dp, rows, columns), bf16),
            pltpu.VMEM((n_dp, rows, columns), bf16),
            pltpu.VMEM((3, chunk_dp, rows, columns), bf16),
            pltpu.VMEM((4, rows, 128), f32),
            pltpu.VMEM((rows, width), f32),
            pltpu.VMEM((rows, width), bf16),
            pltpu.VMEM((n_dp, rows, width), bf16),
            pltpu.VMEM(gate_up.shape, bf16),
            pltpu.VMEM(down_proj.shape, bf16),
            pltpu.VMEM((lanes, chunk_rows), f32),
            pltpu.VMEM((lanes, chunk_rows), f32),
            pltpu.VMEM((n_x, locals_ * slots, chunk_rows), bf16),
            pltpu.VMEM((n_x, locals_ * slots, 128), f32),
            pltpu.VMEM((n_x, 2 * slots, 2 * hidden), bf16),
            pltpu.VMEM((2 * slots, 2 * hidden), f32),
            pltpu.VMEM((2, slots, 2 * hidden), bf16),
            pltpu.VMEM((2 * slots, 2 * hidden), bf16),
            pltpu.VMEM((2 * slots, 2 * hidden), bf16),
            pltpu.VMEM((n_x, 2, slots, hidden), bf16),
            pltpu.VMEM((2, chips, rows, width), bf16),
            pltpu.VMEM((chips, rows, width), bf16),
            pltpu.VMEM((half_r, rows, width), bf16),
            pltpu.VMEM((half_l, rows, width), bf16),
            pltpu.VMEM((half_r, rows, width), bf16),
            pltpu.VMEM((half_l, rows, width), bf16),
            dma((2,)),
            dma((n_dp,)),
            dma((n_dp,)),
            dma((3,)),
            dma((3,)),
            dma((3,)),
            dma((3,)),
            dma((6,)),
            dma((6,)),
            dma((6,)),
            dma((6,)),
            dma((n_x,)),
            dma((n_x,)),
            dma((half_r, 2)),
            dma((half_r, 2)),
            dma((half_l, 2)),
            dma((half_l, 2)),
            *gather_sems,
            *gather_sems,
        ],
        compiler_params=pltpu.CompilerParams(
            collective_id=0, has_side_effects=True, vmem_limit_bytes=56 * 1024 * 1024
        ),
    )(attended, residual, gain, out_weight, gate_up, down_proj)


def mix_columns(expert_ids, route_weights, expert_total):
    share = route_weights / jnp.sum(route_weights, axis=2, keepdims=True)
    catalog = jnp.arange(expert_total, dtype=jnp.int32)
    dense = jnp.sum(jnp.where(expert_ids[..., None] == catalog, share[..., None], 0.0), axis=2)
    dense = dense.reshape(-1, expert_total)
    top = dense.astype(jnp.bfloat16)
    rest = (dense - top.astype(jnp.float32)).astype(jnp.bfloat16)
    return jnp.concatenate([top, rest], axis=1)


def body(
    queries,
    fresh_kv,
    kv_pool,
    page_table,
    context_lengths,
    residual,
    out_weight,
    norm_gain,
    expert_ids,
    route_weights,
    gate_up,
    down_proj,
):
    attended = attend(queries, fresh_kv, kv_pool, page_table, context_lengths)
    step_count, req_count, head_cols = attended.shape
    flat_attended = attended.reshape(step_count * req_count, head_cols)
    dp_count = lax.axis_size("dp")
    local_experts = gate_up.shape[0]
    expert_total = local_experts * dp_count
    top_count = expert_ids.shape[2]
    capacity = min(
        req_count, max(2, (5 * req_count * top_count + 2 * expert_total - 1) // (2 * expert_total))
    )
    quarter = residual.shape[2]
    block = jnp.concatenate(
        [flat_attended, mix_columns(expert_ids, route_weights, expert_total)], axis=1
    )
    out = layer(
        block,
        residual.reshape(step_count * req_count, quarter),
        norm_gain[None, :],
        out_weight,
        gate_up,
        down_proj,
        capacity,
        step_count,
    )
    return out.reshape(step_count, req_count, quarter).astype(jnp.bfloat16)


def solution(mesh):
    return jax.shard_map(
        body,
        mesh=mesh,
        in_specs=(
            P(None, ("groups", "dp"), "expert", None),
            P(None, ("groups", "dp"), "expert", None),
            P(("groups", "dp"), None, "expert", None),
            P(("groups", "dp"), None),
            P(("groups", "dp")),
            P(None, ("groups", "dp"), "expert"),
            P("expert", "dp"),
            P("expert"),
            P(None, ("groups", "dp"), None),
            P(None, ("groups", "dp"), None),
            P("dp", None, "expert", None),
            P("dp", None, "expert"),
        ),
        out_specs=P(None, ("groups", "dp"), "expert"),
        check_vma=False,
    )
```
